32 devices in a mesh: dom: 4 (over z), grp: 8 (over y, x, core).
Axes of the slice: x: 2, y: 2, z: 4, core: 2. Of those that a mesh axis runs over, the one named last changes fastest.
Arguments:
- master_rows: bfloat16 [8, 512, 512], P('grp', 'dom'), may hold values from -6 to 6
- cotangent: bfloat16 [8, 512, 512], P('grp', 'dom'), may hold values from -6 to 6
- relation_weight: bfloat16 [4, 512, 512], replicated, may hold values from -0.125 to 0.125
- self_weight: bfloat16 [512, 512], replicated, may hold values from -0.25 to 0.25
- edge_source: int32 [8, 8192], P('grp', 'dom'), may hold values from 0 to 191
- edge_target: int32 [8, 8192], P('grp', 'dom'), may hold values from 0 to 191
- edge_relation: int32 [8, 8192], P('grp', 'dom'), may hold values from 0 to 3
- send_rows: int32 [8, 256], P('grp', 'dom'), may hold values from 0 to 127
- send_counts: int32 [8, 16], P('grp', 'dom'), may hold values from 4 to 16, as said below
Outputs:
- activation: bfloat16 [8, 512, 512], P('grp', 'dom')
- input_grad: bfloat16 [8, 512, 512], P('grp', 'dom')
- weight_grads: float32 [5, 512, 512], P(None, 'grp')
The draws below stay inside these ranges and needn't reach their ends.
Inputs may be any that keep to these rules, and one draw needn't show every extreme that they name: `send_counts`: on every device the count for some peer is exactly 16.
All inputs are finite; a program needn't handle non-finite values.
Results may differ from the reference program's by a relative error of at most 0.0061.
Values may be sent and summed in bfloat16 or wider, within the bound.
No kernel may reach another device: no remote copies, remote signals or barrier semaphores. Data moves between devices by JAX's collectives and lax.ppermute only.
A program may use at most 64 MiB of HBM per device.

```python
import jax
import jax.numpy as jnp
from jax import lax

D = 512
REL = 4
MAST = 128
CAP = 16
EDGES = 2048
ROWS = 192
N_DOM = 4
N_GRP = 8


def draw_send_counts(key, part):
    key_a, key_b = jax.random.split(jax.random.fold_in(key, 17))
    halvings = jax.random.randint(key_a, (N_GRP, N_DOM, N_DOM), 0, 3)
    counts = jnp.right_shift(jnp.full((N_GRP, N_DOM, N_DOM), CAP, jnp.int32), halvings)
    busiest = jax.random.randint(key_b, (N_GRP, N_DOM, 1), 0, N_DOM)
    counts = jnp.where(jnp.arange(N_DOM)[None, None, :] == busiest, CAP, counts)
    return counts.reshape(N_GRP, N_DOM * N_DOM).astype(jnp.int32)


def touch_ends(result, rng, least, top_value):
    shape = result.shape
    place = [jax.random.randint(jax.random.fold_in(rng, axis), (), 0, shape[axis]) for axis in range(len(shape))]
    result = result.at[tuple(place)].set(least)
    longest = shape.index(max(shape))
    place[longest] = (place[longest] + 1) % shape[longest]
    return result.at[tuple(place)].set(top_value)


def steps_of(rng, extent, cuts, smallest, top_value):
    def one(axis_at, blocks):
        heights = jax.random.uniform(jax.random.fold_in(jax.random.fold_in(rng, 6), axis_at), (blocks,), jnp.float32, smallest / len(cuts), top_value / len(cuts))
        return jnp.repeat(jnp.exp(heights), extent[axis_at] // blocks).reshape((-1,) + (1,) * (len(extent) - axis_at - 1))

    level = one(*cuts[0])
    for cut in cuts[1:]:
        level = level * one(*cut)
    return level


def bell_draw(own_key, dims, spread, limit, shards=(), held_as=jnp.bfloat16):
    array = spread * jax.random.normal(own_key, dims, jnp.float32)
    if shards:
        array = array * steps_of(own_key, dims, shards, -0.22, 0.18)
    return jnp.clip(array, -limit, limit).astype(held_as)


def setup_inputs(seed: int = 0) -> dict:
    seeds = jax.random.split(jax.random.key(seed), 10)
    master_rows = bell_draw(seeds[0], (N_GRP, N_DOM * MAST, D), 1.0, 6.0, ((0, 8), (1, 4)))
    cotangent = bell_draw(seeds[1], (N_GRP, N_DOM * MAST, D), 1.0, 6.0, ((0, 8), (1, 4)))
    relation_weight = bell_draw(seeds[2], (REL, D, D), (4 * D) ** -0.5, 0.125)
    self_weight = bell_draw(seeds[3], (D, D), D ** -0.5, 0.25)
    edge_source = touch_ends(jax.random.randint(seeds[4], (N_GRP, N_DOM * EDGES), 0, ROWS), jax.random.fold_in(seeds[4], 1), 0, ROWS - 1).astype(jnp.int32)
    edge_target = touch_ends(jax.random.randint(seeds[5], (N_GRP, N_DOM * EDGES), 0, ROWS), jax.random.fold_in(seeds[5], 1), 0, ROWS - 1).astype(jnp.int32)
    edge_relation = touch_ends(jax.random.randint(seeds[6], (N_GRP, N_DOM * EDGES), 0, REL), jax.random.fold_in(seeds[6], 1), 0, REL - 1).astype(jnp.int32)
    send_rows = touch_ends(jax.random.randint(seeds[7], (N_GRP, N_DOM * N_DOM * CAP), 0, MAST), jax.random.fold_in(seeds[7], 1), 0, MAST - 1).astype(jnp.int32)
    send_counts = draw_send_counts(jax.random.fold_in(seeds[9], 71), 0)
    return dict(master_rows=master_rows, cotangent=cotangent, relation_weight=relation_weight, self_weight=self_weight, edge_source=edge_source, edge_target=edge_target, edge_relation=edge_relation, send_rows=send_rows, send_counts=send_counts)


def aggregate(table, gather_index, segment_index):
    terms = table[gather_index].astype(jnp.float32)
    summed = jax.ops.segment_sum(terms, segment_index, num_segments=REL * ROWS)
    return summed.reshape(REL, ROWS, D).astype(jnp.bfloat16)


def reference(master_rows, cotangent, relation_weight, self_weight, edge_source, edge_target, edge_relation, send_rows, send_counts):
    weights = relation_weight.astype(jnp.float32)
    masters = master_rows.reshape(N_GRP, N_DOM, MAST, D)
    cotan = cotangent.reshape(N_GRP, N_DOM, MAST, D)
    slots = send_rows.reshape(N_GRP, N_DOM, N_DOM * CAP)
    counts = send_counts.reshape(N_GRP, N_DOM, N_DOM)
    valid = (jnp.arange(CAP)[None, None, None, :] < counts[..., None]).reshape(N_GRP, N_DOM, N_DOM * CAP)
    sources = edge_source.reshape(N_GRP * N_DOM, EDGES)
    targets = edge_target.reshape(N_GRP * N_DOM, EDGES)
    relations = edge_relation.reshape(N_GRP * N_DOM, EDGES)

    def pick(table, index):
        return table[index]

    def pull(table):
        picked = jax.vmap(jax.vmap(pick))(table, slots)
        picked = jnp.where(valid[..., None], picked, jnp.zeros_like(picked))
        picked = picked.reshape(N_GRP, N_DOM, N_DOM, CAP, D).transpose(0, 2, 1, 3, 4).reshape(N_GRP, N_DOM, N_DOM * CAP, D)
        return jnp.concatenate([table, picked], axis=2)

    def add_rows(terms, index):
        return jax.ops.segment_sum(terms, index, num_segments=MAST)

    def push(parts, own):
        moved = parts.reshape(N_GRP, N_DOM, N_DOM, CAP, D).transpose(0, 2, 1, 3, 4).reshape(N_GRP, N_DOM, N_DOM * CAP, D)
        terms = jnp.where(valid[..., None], moved.astype(jnp.float32), 0.0)
        return own + jax.vmap(jax.vmap(add_rows))(terms, slots)

    table = pull(masters).reshape(N_GRP * N_DOM, ROWS, D)
    flat_masters = masters.reshape(N_GRP * N_DOM, MAST, D)

    def forward_device(inputs):
        rows, master, source, target, relation = inputs
        aggregated = aggregate(rows, source, relation * ROWS + target)
        partial_value = jnp.einsum("rnd,rde->ne", aggregated.astype(jnp.float32), weights)
        own = partial_value[:MAST] + jnp.dot(master, self_weight, preferred_element_type=jnp.float32)
        return own, partial_value[MAST:].astype(jnp.bfloat16)

    own, mirror_part = lax.map(forward_device, (table, flat_masters, sources, targets, relations))
    z_value = push(mirror_part.reshape(N_GRP, N_DOM, N_DOM * CAP, D), own.reshape(N_GRP, N_DOM, MAST, D))
    activation = jax.nn.silu(z_value).astype(jnp.bfloat16)
    sigmoid_z = jax.nn.sigmoid(z_value)
    grad_z = (cotan.astype(jnp.float32) * sigmoid_z * (1.0 + z_value * (1.0 - sigmoid_z))).astype(jnp.bfloat16)
    grad_table = pull(grad_z).reshape(N_GRP * N_DOM, ROWS, D)
    flat_grad = grad_z.reshape(N_GRP * N_DOM, MAST, D)

    def backward_device(total, inputs):
        rows, master, grad_rows, grad_master, source, target, relation = inputs
        aggregated = aggregate(rows, source, relation * ROWS + target)
        relation_grad = jnp.einsum("rnd,ne->rde", aggregated.astype(jnp.float32), grad_rows.astype(jnp.float32))
        self_grad = jnp.dot(master.T, grad_master, preferred_element_type=jnp.float32)
        back = aggregate(grad_rows, target, relation * ROWS + source)
        back_partial = jnp.einsum("rne,rde->nd", back.astype(jnp.float32), weights)
        back_own = back_partial[:MAST] + jnp.dot(grad_master, self_weight.T, preferred_element_type=jnp.float32)
        total = total + jnp.concatenate([relation_grad, self_grad[None]], axis=0)
        return total, (back_own, back_partial[MAST:].astype(jnp.bfloat16))

    start = jnp.zeros((REL + 1, D, D), jnp.float32)
    weight_grads, (back_own, back_mirror) = lax.scan(backward_device, start, (table, flat_masters, grad_table, flat_grad, sources, targets, relations))
    input_grad = push(back_mirror.reshape(N_GRP, N_DOM, N_DOM * CAP, D), back_own.reshape(N_GRP, N_DOM, MAST, D))
    activation = activation.reshape(N_GRP, N_DOM * MAST, D)
    input_grad = input_grad.astype(jnp.bfloat16).reshape(N_GRP, N_DOM * MAST, D)
    return activation, input_grad, weight_grads
```

```python
import functools
import math

import jax
import jax.numpy as jnp
from jax import lax
from jax.experimental import pallas as pl
from jax.experimental.pallas import tpu as pltpu
from jax.sharding import PartitionSpec as P

LANES = 128
BF16 = jnp.bfloat16
F32 = jnp.float32
VMEM_LIMIT = 60 * 1024 * 1024
COUNTS_LIMIT = 8 * 1024 * 1024


def dot(a, b):
    return lax.dot_general(a, b, (((1,), (0,)), ((), ())), preferred_element_type=F32)


def dot_nt(a, b):
    return lax.dot_general(a, b, (((1,), (1,)), ((), ())), preferred_element_type=F32)


def dot_tn(a, b):
    return lax.dot_general(a, b, (((0,), (0,)), ((), ())), preferred_element_type=F32)


def one_hot_columns(count, index_row):
    rows = lax.broadcasted_iota(jnp.int32, (count, index_row.shape[1]), 0)
    return jnp.where(rows == index_row, 1.0, 0.0).astype(BF16)


def counts_kernel(edges_ref, map_ref, counts_ref, own_ref, mirror_ref, *, domains, masters, relations):
    local = map_ref.shape[2]
    total = domains * masters
    mirrors = local - masters
    spread = []
    for p in range(domains):
        sources = edges_ref[p, 0:1, :]
        flat = edges_ref[p, 2:3, :] * local + edges_ref[p, 1:2, :]
        local_counts = dot_nt(
            one_hot_columns(relations * local, flat), one_hot_columns(local, sources)
        ).astype(BF16)
        place = one_hot_columns(total, map_ref[p])
        spread.append(place[:, masters:])
        wide = dot_nt(local_counts, place).astype(BF16)
        for r in range(relations):
            base = r * local
            counts_ref[r, p * masters : (p + 1) * masters, :] = wide[base : base + masters]
            mirror_ref[r, p * mirrors : (p + 1) * mirrors, :] = wide[base + masters : base + local]
    spread = jnp.concatenate(spread, axis=1)
    for r in range(relations):
        for p in range(domains):
            rows = slice(p * masters, (p + 1) * masters)
            full = counts_ref[r, rows, :].astype(F32) + dot(spread[rows], mirror_ref[r])
            full = full.astype(BF16)
            counts_ref[r, rows, :] = full
            own_ref[rows, r * masters : (r + 1) * masters] = full[:, :masters]


def forward_kernel(
    counts_ref, table_ref, cotan_ref, weight_ref, self_ref, weight_slice_ref, self_slice_ref,
    active_ref, grad_ref, weight_grad_ref, *, masters, relations,
):
    table = table_ref[...]
    width = cotan_ref.shape[1]
    z_slice = dot(table, self_slice_ref[...])
    z_own = dot(table[:masters], self_ref[...])
    aggregated = []
    for r in range(relations):
        part = dot(counts_ref[r], table).astype(BF16)
        aggregated.append(part)
        z_slice = z_slice + dot(part, weight_slice_ref[r])
    sig = jax.nn.sigmoid(z_slice)
    grad = (cotan_ref[...].astype(F32) * sig * (1.0 + z_slice * (1.0 - sig))).astype(BF16)
    grad_ref[...] = grad
    for r, left in enumerate(aggregated + [table]):
        turned = dot_tn(grad, left)
        weight_grad_ref[:, r * width : (r + 1) * width] = turned.T.astype(BF16)
    for r in range(relations):
        z_own = z_own + dot(aggregated[r][:masters], weight_ref[r])
    active_ref[...] = (z_own * jax.nn.sigmoid(z_own)).astype(BF16)


def backward_kernel(own_ref, grad_ref, weight_ref, self_ref, out_ref, *, masters, relations):
    grad = grad_ref[...]
    back = dot_tn(own_ref[...], grad).astype(BF16)
    total = dot_nt(grad[:masters], self_ref[...])
    for r in range(relations):
        total = total + dot_nt(back[r * masters : (r + 1) * masters], weight_ref[r])
    out_ref[...] = total.astype(BF16)


def assemble_kernel(turn_ref, parts_ref, out_ref):
    pieces = parts_ref.shape[0]
    relations = out_ref.shape[0]
    width = out_ref.shape[2] // pieces
    for c in range(pieces):
        k = turn_ref[c]
        for r in range(relations):
            out_ref[r, :, c * width : (c + 1) * width] = parts_ref[
                k, :, r * width : (r + 1) * width
            ].astype(F32)


def pull_rows(table, send_rows, valid):
    domains = lax.axis_size("dom")
    width = table.shape[1]
    picked = table[send_rows]
    picked = jnp.where(valid[:, None], picked, jnp.zeros_like(picked))
    moved = lax.all_to_all(
        picked.reshape(domains, -1, width), "dom", split_axis=0, concat_axis=0, tiled=True
    )
    return jnp.concatenate([table, moved.reshape(-1, width)], axis=0)


def push_rows(mirror_part, placement, own):
    domains = lax.axis_size("dom")
    width = own.shape[1]
    moved = lax.all_to_all(
        mirror_part.reshape(domains, -1, width), "dom", split_axis=0, concat_axis=0, tiled=True
    )
    return own + jnp.dot(placement, moved.reshape(-1, width), preferred_element_type=jnp.float32)


def edge_counts(sources, targets, relation, relations, local_rows):
    flat_index = (relation * local_rows + targets) * local_rows + sources
    ones = jnp.ones(sources.shape, jnp.float32)
    counted = jax.ops.segment_sum(
        ones, flat_index, num_segments=relations * local_rows * local_rows
    )
    return counted.reshape(relations, local_rows, local_rows).astype(jnp.bfloat16)


def exchange_program(
    master_rows,
    cotangent,
    relation_weight,
    self_weight,
    edge_source,
    edge_target,
    edge_relation,
    send_rows,
    send_counts,
):
    masters = master_rows[0]
    cotan = cotangent[0]
    sources = edge_source[0]
    targets = edge_target[0]
    relation = edge_relation[0]
    slots = send_rows[0]
    counts = send_counts[0]
    domains = lax.axis_size("dom")
    relations = relation_weight.shape[0]
    master_count = masters.shape[0]
    capacity = slots.shape[0] // domains
    valid = (jnp.arange(capacity)[None, :] < counts[:, None]).reshape(-1)
    placement = ((slots[None, :] == jnp.arange(master_count)[:, None]) & valid[None, :]).astype(
        jnp.bfloat16
    )
    table = pull_rows(masters, slots, valid)
    local_rows = table.shape[0]
    adjacency = edge_counts(sources, targets, relation, relations, local_rows)
    aggregated = jnp.einsum(
        "rij,jd->rid", adjacency, table, preferred_element_type=jnp.float32
    ).astype(jnp.bfloat16)
    partial_value = jnp.einsum(
        "rnd,rde->ne", aggregated, relation_weight, preferred_element_type=jnp.float32
    )
    own = partial_value[:master_count] + jnp.dot(
        masters, self_weight, preferred_element_type=jnp.float32
    )
    z_value = push_rows(partial_value[master_count:].astype(jnp.bfloat16), placement, own)
    activation = jax.nn.silu(z_value).astype(jnp.bfloat16)
    sigmoid_z = jax.nn.sigmoid(z_value)
    grad_z = (cotan.astype(jnp.float32) * sigmoid_z * (1.0 + z_value * (1.0 - sigmoid_z))).astype(
        jnp.bfloat16
    )
    grad_table = pull_rows(grad_z, slots, valid)
    relation_grad = jnp.einsum(
        "rnd,ne->rde", aggregated, grad_table, preferred_element_type=jnp.float32
    )
    self_grad = jnp.dot(masters.T, grad_z, preferred_element_type=jnp.float32)
    local_grads = jnp.concatenate([relation_grad, self_grad[None]], axis=0)
    group_part = lax.psum_scatter(local_grads, "grp", scatter_dimension=1, tiled=True)
    weight_grads = lax.psum(group_part, "dom")
    back = jnp.einsum(
        "rij,id->rjd", adjacency, grad_table, preferred_element_type=jnp.float32
    ).astype(jnp.bfloat16)
    back_partial = jnp.einsum(
        "rne,rde->nd", back, relation_weight, preferred_element_type=jnp.float32
    )
    back_own = back_partial[:master_count] + jnp.dot(
        grad_z, self_weight.T, preferred_element_type=jnp.float32
    )
    input_grad = push_rows(back_partial[master_count:].astype(jnp.bfloat16), placement, back_own)
    return (activation[None], input_grad.astype(jnp.bfloat16)[None], weight_grads)


def vmem():
    return pl.BlockSpec(memory_space=pltpu.VMEM)


def call(kernel, outs, args, flops, scratch=(), smem=0):
    specs = [pl.BlockSpec(memory_space=pltpu.SMEM)] * smem + [vmem()] * (len(args) - smem)
    return pl.pallas_call(
        kernel,
        out_shape=outs,
        in_specs=specs,
        out_specs=jax.tree.map(lambda _: vmem(), outs),
        scratch_shapes=list(scratch),
        cost_estimate=pl.CostEstimate(flops=flops, bytes_accessed=1 << 20, transcendentals=0),
        compiler_params=pltpu.CompilerParams(vmem_limit_bytes=VMEM_LIMIT),
    )(*args)


def shift(value, axis, step):
    size = lax.axis_size(axis)
    return lax.ppermute(value, axis, [(i, (i - step) % size) for i in range(size)])


def swap(value, axis, mask):
    return lax.ppermute(value, axis, [(i, i ^ mask) for i in range(lax.axis_size(axis))])


def reduce_over_groups(grads):
    groups = lax.axis_size("grp")
    index = lax.axis_index("grp")
    rows = grads.shape[0] // groups
    shape = (groups, rows, grads.shape[1])
    blocks = grads.reshape(shape)
    if groups % 8:
        moved = lax.all_to_all(blocks, "grp", split_axis=0, concat_axis=0, tiled=True)
        return moved.astype(F32).sum(0)
    core = index % 2
    pairs = blocks.reshape(groups // 2, 2, rows, shape[2])
    keep = lax.dynamic_index_in_dim(pairs, core, 1, keepdims=False)
    give = lax.dynamic_index_in_dim(pairs, 1 - core, 1, keepdims=False)
    both = keep.astype(F32) + swap(give, "grp", 1).astype(F32)
    rounded = both.astype(BF16)
    chip = index // 2
    total = lax.dynamic_index_in_dim(both, chip, 0, keepdims=False)
    if groups == 8:
        for mask in (3, 1, 2):
            total = total + swap(
                lax.dynamic_index_in_dim(rounded, chip ^ mask, 0, keepdims=False), "grp", 2 * mask
            ).astype(F32)
        return total
    chips = groups // 2
    lists = [[2 * c + k for c in range(chips)] for k in range(2)]
    moved = lax.all_to_all(
        rounded, "grp", split_axis=0, concat_axis=0, axis_index_groups=lists, tiled=True
    )
    return moved.astype(F32).sum(0)


def gathered_program(
    master_rows, cotangent, relation_weight, self_weight,
    edge_source, edge_target, edge_relation, send_rows, send_counts,
):
    masters = master_rows[0]
    cotan = cotangent[0]
    slots = send_rows[0]
    used = send_counts[0]
    domains = lax.axis_size("dom")
    place = lax.axis_index("dom")
    relations = relation_weight.shape[0]
    count, depth = masters.shape
    capacity = slots.shape[0] // domains
    local = count + domains * capacity
    edges = edge_source.shape[1]
    total = domains * count
    pieces = math.gcd(domains, depth // LANES)
    width = depth // pieces
    piece = place % pieces

    sends = jnp.concatenate([slots, used, jnp.zeros((edges - slots.shape[0] - domains,), jnp.int32)])
    sheet = jnp.stack([edge_source[0], edge_target[0], edge_relation[0], sends]).astype(jnp.int16)
    sheets = [sheet] + [shift(sheet, "dom", k) for k in range(1, domains)]
    tables = [masters] + [shift(masters, "dom", k) for k in range(1, domains)]
    cuts = [
        lax.dynamic_slice_in_dim(cotan, ((place - k) % pieces) * width, width, 1)
        for k in range(domains)
    ]
    cuts = [cuts[0]] + [shift(cuts[k], "dom", k) for k in range(1, domains)]

    sheet_all = jnp.stack(sheets).astype(jnp.int32)
    slot_all = sheet_all[:, 3, : slots.shape[0]].reshape(domains, domains, capacity)
    used_all = sheet_all[:, 3, slots.shape[0] : slots.shape[0] + domains]
    live = jnp.arange(capacity)[None, None, :] < used_all[:, :, None]
    owner = jnp.arange(domains)[:, None, None] * count
    mirror_of = jnp.where(live, owner + slot_all, -1)
    mirror_of = jnp.roll(jnp.roll(mirror_of, place, axis=0), -place, axis=1)
    mirror_of = mirror_of.transpose(1, 0, 2).reshape(domains, domains * capacity)
    own_map = jnp.arange(domains)[:, None] * count + jnp.arange(count)[None, :]
    row_map = jnp.concatenate([own_map, mirror_of], axis=1).reshape(domains, 1, local)

    counts, own_counts = call(
        functools.partial(counts_kernel, domains=domains, masters=count, relations=relations),
        (
            jax.ShapeDtypeStruct((relations, total, total), BF16),
            jax.ShapeDtypeStruct((total, relations * count), BF16),
        ),
        (sheet_all, row_map),
        2 * domains * relations * local * local * edges,
        scratch=(pltpu.VMEM((relations, domains * domains * capacity, total), BF16),),
    )
    weight_slice = lax.dynamic_slice_in_dim(relation_weight, piece * width, width, 2)
    self_slice = lax.dynamic_slice_in_dim(self_weight, piece * width, width, 1)
    active, grad, weight_grad = call(
        functools.partial(forward_kernel, masters=count, relations=relations),
        (
            jax.ShapeDtypeStruct((count, depth), BF16),
            jax.ShapeDtypeStruct((total, width), BF16),
            jax.ShapeDtypeStruct((depth, (relations + 1) * width), BF16),
        ),
        (
            counts, jnp.concatenate(tables), jnp.concatenate(cuts), relation_weight, self_weight,
            weight_slice, self_slice,
        ),
        2 * relations * total * total * depth,
    )

    grads = [grad]
    for k in range(1, pieces):
        grads.append(jnp.roll(shift(grad, "dom", k), k * count, axis=0))
    grad_full = jnp.concatenate(
        [lax.select_n((c - piece) % pieces, *grads) for c in range(pieces)], axis=1
    )
    input_grad = call(
        functools.partial(backward_kernel, masters=count, relations=relations),
        jax.ShapeDtypeStruct((count, depth), BF16),
        (own_counts, grad_full, relation_weight, self_weight),
        2 * relations * total * count * depth,
    )

    mine = reduce_over_groups(weight_grad).astype(BF16)
    parts = jnp.stack([mine] + [shift(mine, "dom", k) for k in range(1, pieces)])
    turn = (jnp.arange(pieces, dtype=jnp.int32) - piece) % pieces
    weight_grads = call(
        assemble_kernel,
        jax.ShapeDtypeStruct((relations + 1, mine.shape[0], depth), F32),
        (turn, parts),
        1,
        smem=1,
    )
    return active[None], input_grad[None], weight_grads


def per_device(*args):
    relations = args[2].shape[0]
    total = lax.axis_size("dom") * args[0].shape[1]
    table_bytes = 2 * relations * total * total
    form = gathered_program if table_bytes <= COUNTS_LIMIT else exchange_program
    return form(*args)


def solution(mesh):
    return jax.shard_map(
        per_device,
        mesh=mesh,
        in_specs=(
            P("grp", "dom", None),
            P("grp", "dom", None),
            P(),
            P(),
            P("grp", "dom"),
            P("grp", "dom"),
            P("grp", "dom"),
            P("grp", "dom"),
            P("grp", "dom"),
        ),
        out_specs=(P("grp", "dom", None), P("grp", "dom", None), P(None, "grp", None)),
        check_vma=False,
    )
```

```python
import functools

import jax
import jax.numpy as jnp
from jax import lax
from jax.experimental import pallas as pl
from jax.experimental.pallas import tpu as pltpu
from jax.sharding import PartitionSpec as P

LANES = 128
TILE = 16
BF16 = jnp.bfloat16
F32 = jnp.float32
VMEM_LIMIT = 20 * 1024 * 1024
COUNTS_LIMIT = 8 * 1024 * 1024


def dot(a, b):
    return lax.dot_general(a, b, (((1,), (0,)), ((), ())), preferred_element_type=F32)


def dot_nt(a, b):
    return lax.dot_general(a, b, (((1,), (1,)), ((), ())), preferred_element_type=F32)


def dot_tn(a, b):
    return lax.dot_general(a, b, (((0,), (0,)), ((), ())), preferred_element_type=F32)


def one_hot_columns(count, index_row):
    rows = lax.broadcasted_iota(jnp.int32, (count, index_row.shape[1]), 0)
    return jnp.where(rows == index_row, 1.0, 0.0).astype(BF16)


def packet_kernel(
    where_ref, used_ref, cotan_ref, source_ref, target_ref, relation_ref, slot_ref, *packet_refs, capacity
):
    domains = len(packet_refs)
    masters = cotan_ref.shape[0]
    edges = source_ref.shape[1]
    mirrors = domains * capacity
    place = where_ref[0]
    pieces = cotan_ref.shape[1] // LANES

    def renumber(rows):
        turned = rows - capacity * place
        turned = jnp.where(turned < masters, turned + mirrors, turned)
        return jnp.where(rows >= masters, turned, rows)

    lane = lax.broadcasted_iota(jnp.int32, (1, mirrors), 1)
    live = jnp.zeros((1, mirrors), jnp.int32)
    for p in range(domains):
        live = jnp.where((lane >= p * capacity) & (lane < p * capacity + used_ref[0, p]), 1, live)
    slot = jnp.where(live == 1, slot_ref[...], -1)
    turned = slot
    for q in range(1, domains):
        cut = q * capacity
        turned = jnp.where(place == q, jnp.concatenate([slot[:, cut:], slot[:, :cut]], axis=1), turned)
    rows = [renumber(source_ref[...]), renumber(target_ref[...]), relation_ref[...]]
    sheet = [
        row[:, j * LANES : (j + 1) * LANES] for row in rows for j in range(edges // LANES)
    ]
    sheet.append(jnp.concatenate([turned, jnp.zeros((1, LANES - mirrors), jnp.int32)], axis=1))
    sheet.append(jnp.zeros((-len(sheet) % TILE, LANES), jnp.int32))
    sheet = jnp.concatenate(sheet, axis=0).astype(F32).astype(BF16)
    for k, packet_ref in enumerate(packet_refs):
        column = pl.multiple_of(((place + pieces * domains - k) % pieces) * LANES, LANES)
        packet_ref[:masters, :] = cotan_ref[:, pl.ds(column, LANES)]
        packet_ref[masters:, :] = sheet


def counts_kernel(
    *refs, masters, relations, capacity, edges
):
    counts_ref, own_ref, source_ref, target_ref, mirror_ref = refs[-5:]
    packet_refs = refs[:-5]
    domains = len(packet_refs)
    total = domains * masters
    mirrors = domains * capacity
    local = masters + mirrors
    lines = edges // LANES
    row_of = lax.broadcasted_iota(jnp.int32, (local, LANES), 0).astype(F32).astype(BF16)
    row_of = row_of.reshape(local // TILE, TILE, LANES)
    one = jnp.ones((), BF16)
    zero = jnp.zeros((), BF16)

    def hot(line):
        wide = jnp.broadcast_to(line, (TILE, LANES)).astype(BF16)
        return jnp.where(row_of == wide[None], one, zero).reshape(local, LANES)

    slots = [
        ref[masters + 3 * lines : masters + 3 * lines + 1, :].astype(F32).astype(jnp.int32)
        for ref in packet_refs
    ]
    spread = []
    for p, ref in enumerate(packet_refs):
        source = ref[masters : masters + lines, :].astype(F32)
        target = ref[masters + lines : masters + 2 * lines, :].astype(F32)
        relation = ref[masters + 2 * lines : masters + 3 * lines, :].astype(F32)
        for j in range(lines):
            span = slice(j * LANES, (j + 1) * LANES)
            source_ref[:, span] = hot(source[j : j + 1])
            for r in range(relations):
                chosen = jnp.where(relation[j : j + 1] == r, target[j : j + 1], -1.0)
                target_ref[r * local : (r + 1) * local, span] = hot(chosen)
        local_counts = dot_nt(target_ref[...], source_ref[...]).astype(BF16)
        mirror_of = []
        for j in range(domains):
            owner = (j + p) % domains
            block = (-j) % domains
            slot = slots[owner][:, block * capacity : (block + 1) * capacity]
            mirror_of.append(jnp.where(slot < 0, -1, slot + owner * masters))
        mirror_of = one_hot_columns(total, jnp.concatenate(mirror_of, axis=1))
        spread.append(mirror_of)
        own_rows = p * masters + lax.broadcasted_iota(jnp.int32, (1, masters), 1)
        place = jnp.concatenate([one_hot_columns(total, own_rows), mirror_of], axis=1)
        wide = dot_nt(local_counts, place).astype(BF16)
        for r in range(relations):
            base = r * local
            counts_ref[r, p * masters : (p + 1) * masters, :] = wide[base : base + masters]
            mirror_ref[r, p * mirrors : (p + 1) * mirrors, :] = wide[base + masters : base + local]
    spread = jnp.concatenate(spread, axis=1)
    for r in range(relations):
        full = (counts_ref[r].astype(F32) + dot(spread, mirror_ref[r])).astype(BF16)
        counts_ref[r] = full
        own_ref[:, r * masters : (r + 1) * masters] = full[:, :masters]


def forward_kernel(where_ref, counts_ref, weight_ref, self_ref, *refs, domains, relations):
    piece = where_ref[1]
    core = where_ref[2]
    table_refs = refs[:domains]
    packet_refs = refs[domains : 2 * domains]
    own_ref, grad_ref, keep_ref, give_ref, table_ref, cotan_ref = refs[2 * domains :]
    masters = table_refs[0].shape[0]
    for k in range(domains):
        table_ref[k * masters : (k + 1) * masters, :] = table_refs[k][...]
        cotan_ref[k * masters : (k + 1) * masters, :] = packet_refs[k][:masters, :]
    table = table_ref[...]
    column = pl.multiple_of(piece * LANES, LANES)
    z_slice = dot(table, self_ref[:, pl.ds(column, LANES)])
    aggregated = []
    for r in range(relations):
        part = dot(counts_ref[r], table).astype(BF16)
        aggregated.append(part)
        own_ref[:, r * part.shape[1] : (r + 1) * part.shape[1]] = part[:masters]
        z_slice = z_slice + dot(part, weight_ref[r, :, pl.ds(column, LANES)])
    sig = jax.nn.sigmoid(z_slice)
    grad = (cotan_ref[...].astype(F32) * sig * (1.0 + z_slice * (1.0 - sig))).astype(BF16)
    grad_ref[...] = grad
    chips, rows, _ = keep_ref.shape
    for r, left in enumerate(aggregated + [table]):
        turned = dot_tn(grad, left).T.astype(BF16)
        span = slice(r * LANES, (r + 1) * LANES)
        for parity in range(2):
            blocks = [
                turned[(2 * c + parity) * rows : (2 * c + parity + 1) * rows] for c in range(chips)
            ]

            @pl.when(core == parity)
            def _():
                for c in range(chips):
                    keep_ref[c, :, span] = blocks[c]

            @pl.when(core != parity)
            def _():
                for c in range(chips):
                    give_ref[c, :, span] = blocks[c]


def activation_kernel(own_ref, table_ref, weight_ref, self_ref, out_ref):
    depth = table_ref.shape[1]
    z = dot(table_ref[...], self_ref[...])
    for r in range(weight_ref.shape[0]):
        z = z + dot(own_ref[:, r * depth : (r + 1) * depth], weight_ref[r])
    out_ref[...] = (z * jax.nn.sigmoid(z)).astype(BF16)


def backward_kernel(where_ref, own_ref, weight_ref, self_ref, *refs):
    out_ref, grad_ref = refs[-2:]
    parts = refs[:-2]
    masters = out_ref.shape[0]
    relations = weight_ref.shape[0]
    pieces = len(parts)
    total = grad_ref.shape[0]
    for k, part in enumerate(parts):
        column = pl.multiple_of(((where_ref[1] + k) % pieces) * LANES, LANES)
        moved = k * masters
        grad_ref[moved:, pl.ds(column, LANES)] = part[: total - moved, :]
        if k:
            grad_ref[:moved, pl.ds(column, LANES)] = part[total - moved :, :]
    grad = grad_ref[...]
    back = dot_tn(own_ref[...], grad).astype(BF16)
    out = dot_nt(grad[:masters], self_ref[...])
    for r in range(relations):
        out = out + dot_nt(back[r * masters : (r + 1) * masters], weight_ref[r])
    out_ref[...] = out.astype(BF16)


def assemble_kernel(where_ref, *refs):
    parts, out_ref = refs[:-1], refs[-1]
    for k, part in enumerate(parts):
        column = pl.multiple_of(((where_ref[1] + k) % len(parts)) * LANES, LANES)
        for r in range(out_ref.shape[0]):
            out_ref[r, :, pl.ds(column, LANES)] = part[:, r * LANES : (r + 1) * LANES].astype(F32)


def pull_rows(table, send_rows, valid):
    domains = lax.axis_size("dom")
    width = table.shape[1]
    picked = table[send_rows]
    picked = jnp.where(valid[:, None], picked, jnp.zeros_like(picked))
    moved = lax.all_to_all(
        picked.reshape(domains, -1, width), "dom", split_axis=0, concat_axis=0, tiled=True
    )
    return jnp.concatenate([table, moved.reshape(-1, width)], axis=0)


def push_rows(mirror_part, placement, own):
    domains = lax.axis_size("dom")
    width = own.shape[1]
    moved = lax.all_to_all(
        mirror_part.reshape(domains, -1, width), "dom", split_axis=0, concat_axis=0, tiled=True
    )
    return own + jnp.dot(placement, moved.reshape(-1, width), preferred_element_type=jnp.float32)


def edge_counts(sources, targets, relation, relations, local_rows):
    flat_index = (relation * local_rows + targets) * local_rows + sources
    ones = jnp.ones(sources.shape, jnp.float32)
    counted = jax.ops.segment_sum(
        ones, flat_index, num_segments=relations * local_rows * local_rows
    )
    return counted.reshape(relations, local_rows, local_rows).astype(jnp.bfloat16)


def exchange_program(
    master_rows,
    cotangent,
    relation_weight,
    self_weight,
    edge_source,
    edge_target,
    edge_relation,
    send_rows,
    send_counts,
):
    masters = master_rows[0]
    cotan = cotangent[0]
    sources = edge_source[0]
    targets = edge_target[0]
    relation = edge_relation[0]
    slots = send_rows[0]
    counts = send_counts[0]
    domains = lax.axis_size("dom")
    relations = relation_weight.shape[0]
    master_count = masters.shape[0]
    capacity = slots.shape[0] // domains
    valid = (jnp.arange(capacity)[None, :] < counts[:, None]).reshape(-1)
    placement = ((slots[None, :] == jnp.arange(master_count)[:, None]) & valid[None, :]).astype(
        jnp.bfloat16
    )
    table = pull_rows(masters, slots, valid)
    local_rows = table.shape[0]
    adjacency = edge_counts(sources, targets, relation, relations, local_rows)
    aggregated = jnp.einsum(
        "rij,jd->rid", adjacency, table, preferred_element_type=jnp.float32
    ).astype(jnp.bfloat16)
    partial_value = jnp.einsum(
        "rnd,rde->ne", aggregated, relation_weight, preferred_element_type=jnp.float32
    )
    own = partial_value[:master_count] + jnp.dot(
        masters, self_weight, preferred_element_type=jnp.float32
    )
    z_value = push_rows(partial_value[master_count:].astype(jnp.bfloat16), placement, own)
    activation = jax.nn.silu(z_value).astype(jnp.bfloat16)
    sigmoid_z = jax.nn.sigmoid(z_value)
    grad_z = (cotan.astype(jnp.float32) * sigmoid_z * (1.0 + z_value * (1.0 - sigmoid_z))).astype(
        jnp.bfloat16
    )
    grad_table = pull_rows(grad_z, slots, valid)
    relation_grad = jnp.einsum(
        "rnd,ne->rde", aggregated, grad_table, preferred_element_type=jnp.float32
    )
    self_grad = jnp.dot(masters.T, grad_z, preferred_element_type=jnp.float32)
    local_grads = jnp.concatenate([relation_grad, self_grad[None]], axis=0)
    group_part = lax.psum_scatter(local_grads, "grp", scatter_dimension=1, tiled=True)
    weight_grads = lax.psum(group_part, "dom")
    back = jnp.einsum(
        "rij,id->rjd", adjacency, grad_table, preferred_element_type=jnp.float32
    ).astype(jnp.bfloat16)
    back_partial = jnp.einsum(
        "rne,rde->nd", back, relation_weight, preferred_element_type=jnp.float32
    )
    back_own = back_partial[:master_count] + jnp.dot(
        grad_z, self_weight.T, preferred_element_type=jnp.float32
    )
    input_grad = push_rows(back_partial[master_count:].astype(jnp.bfloat16), placement, back_own)
    return (activation[None], input_grad.astype(jnp.bfloat16)[None], weight_grads)


def call(kernel, outs, args, flops, scratch=(), smem=0):
    args = list(args[:smem]) + [pltpu.with_memory_space_constraint(a, pltpu.VMEM) for a in args[smem:]]
    specs = [pl.BlockSpec(memory_space=pltpu.SMEM)] * smem
    specs += [pl.BlockSpec(memory_space=pltpu.VMEM)] * (len(args) - smem)
    return pl.pallas_call(
        kernel,
        out_shape=outs,
        in_specs=specs,
        out_specs=[pl.BlockSpec(memory_space=pltpu.VMEM)] * len(outs),
        scratch_shapes=list(scratch),
        cost_estimate=pl.CostEstimate(flops=flops, bytes_accessed=1 << 20, transcendentals=0),
        compiler_params=pltpu.CompilerParams(vmem_limit_bytes=VMEM_LIMIT),
    )(*args)


def shift(value, axis, step):
    size = lax.axis_size(axis)
    return lax.ppermute(value, axis, [(i, (i - step) % size) for i in range(size)])


def swap(value, axis, mask):
    return lax.ppermute(value, axis, [(i, i ^ mask) for i in range(lax.axis_size(axis))])


def gathered_program(
    master_rows, cotangent, relation_weight, self_weight,
    edge_source, edge_target, edge_relation, send_rows, send_counts,
):
    masters = master_rows[0]
    domains = lax.axis_size("dom")
    groups = lax.axis_size("grp")
    place = lax.axis_index("dom")
    group = lax.axis_index("grp")
    relations = relation_weight.shape[0]
    count, depth = masters.shape
    capacity = send_rows.shape[1] // domains
    edges = edge_source.shape[1]
    total = domains * count
    pieces = depth // LANES
    mirrors = domains * capacity
    local = count + mirrors
    chips = groups // 2
    rows = depth // groups
    where = jnp.stack([place, place % pieces, group % 2]).astype(jnp.int32)

    sheet_rows = 3 * (edges // LANES) + 1
    packet = pltpu.VMEM((count + sheet_rows + -sheet_rows % TILE, LANES), BF16)
    packets = call(
        functools.partial(packet_kernel, capacity=capacity),
        [packet] * domains,
        (where, send_counts, cotangent[0], edge_source, edge_target, edge_relation, send_rows),
        1 << 20,
        smem=2,
    )
    packets = [packets[0]] + [shift(packets[k], "dom", k) for k in range(1, domains)]
    tables = [masters] + [shift(masters, "dom", k) for k in range(1, domains)]

    counts, own_counts = call(
        functools.partial(
            counts_kernel, masters=count, relations=relations, capacity=capacity, edges=edges
        ),
        [
            pltpu.VMEM((relations, total, total), BF16),
            pltpu.VMEM((total, relations * count), BF16),
        ],
        packets,
        4 * domains * relations * local * local * edges,
        scratch=(
            pltpu.VMEM((local, edges), BF16),
            pltpu.VMEM((relations * local, edges), BF16),
            pltpu.VMEM((relations, domains * mirrors, total), BF16),
        ),
    )
    own_part, grad, keep, give = call(
        functools.partial(forward_kernel, domains=domains, relations=relations),
        [
            pltpu.VMEM((count, relations * depth), BF16),
            pltpu.VMEM((total, LANES), BF16),
            pltpu.VMEM((chips, rows, (relations + 1) * LANES), BF16),
            pltpu.VMEM((chips, rows, (relations + 1) * LANES), BF16),
        ],
        (where, counts, relation_weight, self_weight, *tables, *packets),
        2 * relations * total * total * depth,
        scratch=(pltpu.VMEM((total, depth), BF16), pltpu.VMEM((total, LANES), BF16)),
        smem=1,
    )

    both = keep.astype(F32) + swap(give, "grp", 1).astype(F32)
    both, grad = lax.optimization_barrier((both, grad))
    chip = group // 2
    mine = lax.dynamic_index_in_dim(both, chip, 0, keepdims=False)
    rounded = both.astype(BF16)
    for mask in (3, 1, 2):
        mine = mine + swap(
            lax.dynamic_index_in_dim(rounded, chip ^ mask, 0, keepdims=False), "grp", 2 * mask
        ).astype(F32)
    mine = mine.astype(BF16)

    (active,) = call(
        activation_kernel,
        [jax.ShapeDtypeStruct((count, depth), BF16)],
        (own_part, masters, relation_weight, self_weight),
        2 * relations * count * depth * depth,
    )
    grads = [grad] + [shift(grad, "dom", k) for k in range(1, pieces)]
    (input_grad,) = call(
        backward_kernel,
        [jax.ShapeDtypeStruct((count, depth), BF16)],
        (where, own_counts, relation_weight, self_weight, *grads),
        4 * relations * total * count * depth,
        scratch=(pltpu.VMEM((total, depth), BF16),),
        smem=1,
    )
    parts = [mine] + [shift(mine, "dom", k) for k in range(1, pieces)]
    (weight_grads,) = call(
        assemble_kernel,
        [jax.ShapeDtypeStruct((relations + 1, rows, depth), F32)],
        (where, *parts),
        1,
        smem=1,
    )
    return active[None], input_grad[None], weight_grads


def per_device(*args):
    masters, weights, sources, slots = args[0], args[2], args[4], args[7]
    domains = lax.axis_size("dom")
    total = domains * masters.shape[1]
    fits = (
        weights.shape[1] == domains * LANES
        and lax.axis_size("grp") == 8
        and slots.shape[1] <= LANES
        and sources.shape[1] % (LANES * TILE) == 0
        and masters.shape[1] + slots.shape[1] <= 256
        and weights.shape[0] <= 256
        and 2 * weights.shape[0] * total * total <= COUNTS_LIMIT
    )
    return (gathered_program if fits else exchange_program)(*args)


def solution(mesh):
    return jax.shard_map(
        per_device,
        mesh=mesh,
        in_specs=(
            P("grp", "dom", None),
            P("grp", "dom", None),
            P(),
            P(),
            P("grp", "dom"),
            P("grp", "dom"),
            P("grp", "dom"),
            P("grp", "dom"),
            P("grp", "dom"),
        ),
        out_specs=(P("grp", "dom", None), P("grp", "dom", None), P(None, "grp", None)),
        check_vma=False,
    )
```
